256 devices in a mesh: section: 8 (over z_lo, y), dp: 32 (over x, z_hi, core).
Axes of the slice: x: 4, y: 4, z: 8 (z_hi: 4, z_lo: 2; z = z_hi * 2 + z_lo), core: 2. Of those that a mesh axis runs over, the one named last changes fastest.
Arguments:
- inputs: bfloat16 [256, 128, 1536], P('dp'), parts along dimension 0, may hold values from -6 to 6
- w_query: bfloat16 [8, 1536, 768], P('section'), may hold values from -0.15625 to 0.15625
- w_key: bfloat16 [8, 1536, 768], P('section'), may hold values from -0.15625 to 0.15625
- w_value: bfloat16 [8, 1536, 768], P('section'), may hold values from -0.15625 to 0.15625
- w_out: bfloat16 [8, 768, 1536], P('section'), may hold values from -0.21875 to 0.21875
- mixing: float32 [8], P('section'), may hold values from 0.2 to 0.8
Outputs:
- outputs: bfloat16 [256, 128, 1536], P(('dp', 'section')), parts along dimension 0
The draws below stay inside these ranges and needn't reach their ends.
There are 32 independent parts, one for each index of `dp`. The reference program is written for one: setup_inputs(seed, part) draws one part's arguments, and reference() takes and returns one part's arrays. A program takes and returns all parts, laid end to end along the dimension named above; an argument that names none is the same for every part. Nothing has to cross between parts.
All inputs are finite; a program needn't handle non-finite values.
Results may differ from the reference program's by a relative error of at most 0.023.
Values may be sent and summed in bfloat16 or wider, within the bound.
No kernel may reach another device: no remote copies, remote signals or barrier semaphores. Data moves between devices by JAX's collectives and lax.ppermute only.
A program may use at most 128 MiB of HBM per device.

```python
import jax
import jax.numpy as jnp
from jax import lax

D = 1536
HEADS = 6
HEAD_DIM = 128
SEQ = 128
HD = 768
MICRO = 8
LAYERS = 8


def level_of(stream_key, dims, split, low, top_value):
    def one(position, shards_of):
        draws = jax.random.uniform(jax.random.fold_in(jax.random.fold_in(stream_key, 6), position), (shards_of,), jnp.float32, low / len(split), top_value / len(split))
        return jnp.repeat(jnp.exp(draws), dims[position] // shards_of).reshape((-1,) + (1,) * (len(dims) - position - 1))

    gain = one(*split[0])
    for cut in split[1:]:
        gain = gain * one(*cut)
    return gain


def scatter_about(key, dims, width, reach, pieces=(), kind=jnp.bfloat16):
    entries = jax.random.normal(key, dims, jnp.float32) * width
    if len(pieces) > 0:
        entries = level_of(key, dims, pieces, -0.22, 0.18) * entries
    return jnp.clip(entries, min=-reach, max=reach).astype(kind)


def setup_inputs(seed: int = 0, part: int = 0) -> dict:
    key_of = jax.random.split(jax.random.key(seed), 7)
    part_keys = jax.random.split(jax.random.fold_in(key_of[6], part), 7)
    inputs = scatter_about(part_keys[0], (MICRO, SEQ, D), 1.0, 6.0)
    w_query = scatter_about(key_of[1], (LAYERS, D, HD), D ** -0.5, 0.15625, ((0, 8),))
    w_key = scatter_about(key_of[2], (LAYERS, D, HD), D ** -0.5, 0.15625, ((0, 8),))
    w_value = scatter_about(key_of[3], (LAYERS, D, HD), D ** -0.5, 0.15625, ((0, 8),))
    w_out = scatter_about(key_of[4], (LAYERS, HD, D), HD ** -0.5, 0.21875, ((0, 8),))
    mixing = jnp.clip(0.2 + 0.6 * jax.random.uniform(key_of[5], (LAYERS,), jnp.float32) ** level_of(key_of[5], (LAYERS,), ((0, 8),), -0.2, 0.2), 0.2, 0.8)
    return dict(inputs=inputs, w_query=w_query, w_key=w_key, w_value=w_value, w_out=w_out, mixing=mixing)


epsilon = 1e-06
score_scale = 0.12

def norm_rows(tensor):
    return tensor * lax.rsqrt(lax.optimization_barrier(jnp.mean(tensor * tensor, axis=-1, keepdims=True)) + epsilon)

def layer_apply(hidden, w_query, w_key, w_value, w_out, mixing, first_values, first_flag):
    row_count = hidden.shape[0]
    hidden_wide = hidden.astype(jnp.float32)
    normed = norm_rows(hidden_wide).astype(jnp.bfloat16)
    queries = jnp.dot(normed, w_query, preferred_element_type=jnp.float32).reshape(row_count, HEADS, HEAD_DIM)
    key_rows = jnp.dot(normed, w_key, preferred_element_type=jnp.float32).reshape(row_count, HEADS, HEAD_DIM)
    queries = norm_rows(queries).astype(jnp.bfloat16)
    key_rows = norm_rows(key_rows).astype(jnp.bfloat16)
    values = jnp.dot(normed, w_value, preferred_element_type=jnp.float32)
    own_values = values.astype(jnp.bfloat16)
    if first_flag:
        used_values = own_values
    else:
        used_values = (mixing * values + (1.0 - mixing) * first_values.astype(jnp.float32)).astype(jnp.bfloat16)
    used_values = used_values.reshape(row_count, HEADS, HEAD_DIM)
    scores = jnp.einsum('qhd,khd->hqk', queries.astype(jnp.float32), key_rows.astype(jnp.float32)) * score_scale
    positions = jnp.arange(row_count, dtype=jnp.int32)
    causal = positions[:, None] >= positions[None, :]
    weights = jnp.where(causal[None, :, :], jnp.exp(scores), 0.0)
    probabilities = (weights / lax.optimization_barrier(jnp.sum(weights, axis=-1, keepdims=True))).astype(jnp.bfloat16)
    attended = jnp.einsum('hqk,khd->qhd', probabilities.astype(jnp.float32), used_values.astype(jnp.float32))
    attended = attended.astype(jnp.bfloat16).reshape(row_count, HEADS * HEAD_DIM)
    result = (hidden_wide + jnp.dot(attended, w_out, preferred_element_type=jnp.float32)).astype(jnp.bfloat16)
    return (result, own_values)

def reference(inputs, w_query, w_key, w_value, w_out, mixing):
    finished = []
    for micro_index in range(inputs.shape[0]):
        hidden = inputs[micro_index]
        first_values = None
        for layer_number in range(w_query.shape[0]):
            hidden, own_values = layer_apply(hidden, w_query[layer_number], w_key[layer_number], w_value[layer_number], w_out[layer_number], mixing[layer_number], first_values, layer_number == 0)
            if layer_number == 0:
                first_values = own_values
        finished.append(hidden)
    return jnp.stack(finished)
```

```python
import functools

import jax
import jax.numpy as jnp
from jax import lax
from jax.experimental import pallas as pl
from jax.experimental.pallas import tpu as pltpu
from jax.sharding import PartitionSpec as P

HEADS = 6
CHUNKS = 2

epsilon = 1e-06
score_scale = 0.12


def norm_rows(tensor):
    return tensor * lax.rsqrt(jnp.mean(tensor * tensor, axis=-1, keepdims=True) + epsilon)


def layer_kernel(step, chunk, rows, micro_count, *refs):
    (inputs_ref, received_ref, wq_ref, wk_ref, wv_ref, wo_ref, mix_ref, token_ref) = refs[:8]
    earlier = refs[8 : 8 + 2 * chunk]
    (sent_ref, keys_ref, used_ref, token_out_ref) = refs[8 + 2 * chunk : 12 + 2 * chunk]
    attended_ref = refs[12 + 2 * chunk]
    del token_ref, token_out_ref
    section = lax.axis_index("section")
    micro = step - section
    width = wq_ref.shape[0]
    value_width = wq_ref.shape[1]
    head_dim = value_width // HEADS

    @pl.when(jnp.logical_and(micro >= 0, micro < micro_count))
    def _():
        first_section = section == 0
        fresh = inputs_ref[min(step, micro_count - 1), chunk * rows : (chunk + 1) * rows, :]
        hidden = jnp.where(first_section, fresh, received_ref[:, :width])
        hidden_wide = hidden.astype(jnp.float32)
        normed = norm_rows(hidden_wide).astype(jnp.bfloat16)
        values = jnp.dot(normed, wv_ref[...], preferred_element_type=jnp.float32)
        queries = jnp.dot(normed, wq_ref[...], preferred_element_type=jnp.float32)
        key_rows = jnp.dot(normed, wk_ref[...], preferred_element_type=jnp.float32)
        own = values.astype(jnp.bfloat16)
        first = jnp.where(first_section, own, received_ref[:, width:])
        sent_ref[:, width:] = first
        mix = mix_ref[0:1, 0:1]
        blended = (mix * values + (1.0 - mix) * first.astype(jnp.float32)).astype(jnp.bfloat16)
        used_ref[...] = jnp.where(first_section, own, blended)
        row_ids = lax.broadcasted_iota(jnp.int32, (rows, rows), 0)
        column_ids = lax.broadcasted_iota(jnp.int32, (rows, rows), 1)
        causal = row_ids >= column_ids
        for head in range(HEADS):
            lanes = slice(head * head_dim, (head + 1) * head_dim)
            query = norm_rows(queries[:, lanes]).astype(jnp.bfloat16)
            key = norm_rows(key_rows[:, lanes]).astype(jnp.bfloat16)
            keys_ref[:, lanes] = key
            blocks = [(earlier[2 * i][:, lanes], earlier[2 * i + 1][:, lanes]) for i in range(chunk)]
            blocks.append((key, used_ref[:, lanes]))
            total = 0.0
            weights = []
            for index, (block_keys, _unused) in enumerate(blocks):
                scores = (
                    lax.dot_general(
                        query, block_keys, (((1,), (1,)), ((), ())),
                        preferred_element_type=jnp.float32,
                    )
                    * score_scale
                )
                weight = jnp.exp(scores)
                if index == chunk:
                    weight = jnp.where(causal, weight, 0.0)
                total = total + jnp.sum(weight, axis=-1, keepdims=True)
                weights.append(weight)
            attended = 0.0
            for weight, (_unused, block_values) in zip(weights, blocks):
                probabilities = (weight / total).astype(jnp.bfloat16)
                attended = attended + jnp.dot(
                    probabilities, block_values, preferred_element_type=jnp.float32
                )
            attended_ref[:, lanes] = attended.astype(jnp.bfloat16)
        projected = jnp.dot(attended_ref[...], wo_ref[...], preferred_element_type=jnp.float32)
        sent_ref[:, :width] = (hidden_wide + projected).astype(jnp.bfloat16)


def layer_call(step, chunk, rows, operands):
    inputs, received, w_query = operands[:3]
    micro_count, _, width = inputs.shape
    value_width = w_query.shape[-1]
    vmem = pl.BlockSpec(memory_space=pltpu.VMEM)
    any_space = pl.BlockSpec(memory_space=pl.ANY)
    in_specs = [vmem] * 7 + [any_space] + [vmem] * (2 * chunk)
    return pl.pallas_call(
        functools.partial(layer_kernel, step, chunk, rows, micro_count),
        out_shape=(
            jax.ShapeDtypeStruct((rows, width + value_width), jnp.bfloat16),
            jax.ShapeDtypeStruct((rows, value_width), jnp.bfloat16),
            jax.ShapeDtypeStruct((rows, value_width), jnp.bfloat16),
            jax.ShapeDtypeStruct((8, 128), jnp.float32),
        ),
        in_specs=in_specs,
        out_specs=(vmem, vmem, vmem, any_space),
        scratch_shapes=[pltpu.VMEM((rows, value_width), jnp.bfloat16)],
        compiler_params=pltpu.CompilerParams(vmem_limit_bytes=40 * 1024 * 1024),
        cost_estimate=pl.CostEstimate(
            flops=8 * rows * width * value_width, bytes_accessed=0, transcendentals=0
        ),
        name="layer",
    )(*operands)


def body(inputs, w_query, w_key, w_value, w_out, mixing):
    section_count = lax.axis_size("section")
    section_index = lax.axis_index("section")
    micro_count, row_count, width = inputs.shape
    value_width = w_value.shape[2]
    last_section = section_count - 1
    rows = row_count // CHUNKS
    constants = (w_query[0], w_key[0], w_value[0], w_out[0], jnp.broadcast_to(mixing[:, None], (8, 128)))
    received = [jnp.zeros((rows, width + value_width), jnp.bfloat16)] * CHUNKS
    token = jnp.zeros((8, 128), jnp.float32)
    homes = []
    for step in range(micro_count + section_count - 1):
        arrived = []
        earlier = ()
        for chunk in range(CHUNKS):
            sent, keys, used, token = layer_call(
                step, chunk, rows, (inputs, received[chunk]) + constants + (token,) + earlier
            )
            earlier = earlier + (keys, used)
            pairs = [
                (s, s + 1) for s in range(last_section) if 0 <= step - s < micro_count
            ]
            done = step - last_section
            if 0 <= done < last_section:
                pairs.append((last_section, done))
            arrived.append(lax.ppermute(sent, "section", pairs) if pairs else sent)
        received = arrived
        if step >= last_section:
            homes.append(jnp.concatenate(received, 0)[:, :width])
    output = homes[-1]
    for micro in range(micro_count - 1):
        output = jnp.where(section_index == micro, homes[micro], output)
    return output[None]


def solution(mesh):
    in_specs = (
        P("dp", None, None),
        P("section", None, None),
        P("section", None, None),
        P("section", None, None),
        P("section", None, None),
        P("section"),
    )
    out_specs = P(("dp", "section"), None, None)
    return jax.shard_map(body, mesh=mesh, in_specs=in_specs, out_specs=out_specs, check_vma=False)
```

```python
import functools

import jax
import jax.numpy as jnp
from jax import lax
from jax.experimental import pallas as pl
from jax.experimental.pallas import tpu as pltpu
from jax.sharding import PartitionSpec as P

HEADS = 6
CHUNKS = 2

epsilon = 1e-06
score_scale = 0.12


VMEM = pl.BlockSpec(memory_space=pltpu.VMEM)
ANY = pl.BlockSpec(memory_space=pl.ANY)
HBM = pl.BlockSpec(memory_space=pltpu.HBM)
SCOPED_BYTES = 8 * 1024 * 1024


def norm_rows(tensor):
    return tensor * lax.rsqrt(jnp.mean(tensor * tensor, axis=-1, keepdims=True) + epsilon)


def heads_of(tensor):
    head_dim = tensor.shape[-1] // HEADS
    return [tensor[:, head * head_dim : (head + 1) * head_dim] for head in range(HEADS)]


def dot(left, right):
    return jnp.dot(left, right, preferred_element_type=jnp.float32)


def layer_chunk(hidden, first, is_first, mix, weights, earlier):
    rows = hidden.shape[0]
    wq_ref, wk_ref, wv_ref, wo_ref = weights
    hidden_wide = hidden.astype(jnp.float32)
    normed = norm_rows(hidden_wide).astype(jnp.bfloat16)
    queries = dot(normed, wq_ref[...])
    key_rows = dot(normed, wk_ref[...])
    values = dot(normed, wv_ref[...])
    queries = [norm_rows(head).astype(jnp.bfloat16) for head in heads_of(queries)]
    keys = [norm_rows(head).astype(jnp.bfloat16) for head in heads_of(key_rows)]
    own = values.astype(jnp.bfloat16)
    blended = (mix * values + (1.0 - mix) * first.astype(jnp.float32)).astype(jnp.bfloat16)
    used = jnp.where(is_first, own, blended)
    all_keys, all_used = keys, heads_of(used)
    if earlier is not None:
        all_keys = [jnp.concatenate(pair, 0) for pair in zip(heads_of(earlier[0]), keys)]
        all_used = [jnp.concatenate(pair, 0) for pair in zip(heads_of(earlier[1]), all_used)]
    scores = [
        lax.dot_general(query, key, (((1,), (1,)), ((), ())), preferred_element_type=jnp.float32)
        for query, key in zip(queries, all_keys)
    ]
    count = all_keys[0].shape[0]
    row_ids = lax.broadcasted_iota(jnp.int32, (rows, count), 0) + (count - rows)
    causal = row_ids >= lax.broadcasted_iota(jnp.int32, (rows, count), 1)
    masses = [jnp.where(causal, jnp.exp(score * score_scale), 0.0) for score in scores]
    totals = [jnp.sum(mass, axis=-1, keepdims=True) for mass in masses]
    shares = [(mass / total).astype(jnp.bfloat16) for mass, total in zip(masses, totals)]
    attended = [dot(share, value).astype(jnp.bfloat16) for share, value in zip(shares, all_used)]
    projected = dot(jnp.concatenate(attended, 1), wo_ref[...])
    return (hidden_wide + projected).astype(jnp.bfloat16), keys, used


def start_copies(pairs, semaphores):
    copies = [
        pltpu.make_async_copy(source, target, semaphores.at[index])
        for index, (source, target) in enumerate(pairs)
    ]
    for copy in copies:
        copy.start()
    return copies


def first_values(rows, wv):
    return dot(norm_rows(rows.astype(jnp.float32)).astype(jnp.bfloat16), wv).astype(jnp.bfloat16)


def early_kernel(*refs):
    sources, mixing_ref = refs[:6], refs[6]
    out_ref, mix_ref, _token, _received = refs[7:11]
    targets, semaphores = refs[11:17], refs[17]
    copies = start_copies(list(zip(sources, targets)), semaphores)
    mix_ref[...] = jnp.full(mix_ref.shape, mixing_ref[0])
    copies[0].wait()
    copies[1].wait()

    @pl.when(lax.axis_index("section") == 0)
    def _():
        out_ref[...] = first_values(targets[0][0], targets[1][...])

    for copy in copies[2:]:
        copy.wait()


def early_call(inputs, w_value, w_query, w_key, w_out, mixing, rows):
    micro_count, row_count, width = inputs.shape
    loaded = (inputs, w_value, w_query, w_key, w_out)
    results = pl.pallas_call(
        early_split,
        out_shape=[
            jax.ShapeDtypeStruct((row_count, w_value.shape[1]), jnp.bfloat16),
            pltpu.VMEM((8, 128), jnp.float32),
            jax.ShapeDtypeStruct((8, 128), jnp.float32),
            pltpu.VMEM((rows, width), jnp.bfloat16),
        ]
        + [pltpu.VMEM(w.shape, w.dtype) for w in loaded],
        in_specs=[HBM] * 5 + [pl.BlockSpec(memory_space=pltpu.SMEM)],
        out_specs=[VMEM, VMEM, ANY, VMEM] + [VMEM] * 5,
        scratch_shapes=[pltpu.SemaphoreType.DMA((6,))],
        compiler_params=pltpu.CompilerParams(vmem_limit_bytes=50 * 1024 * 1024),
        name="early",
    )(*loaded, mixing)
    return results


def early_split(*refs):
    inputs, others, mixing = refs[0], refs[1:5], refs[5]
    plain, inputs_out, others_out, semaphores = refs[6:10], refs[10], refs[11:15], refs[15]
    rest = pl.ds(1, inputs.shape[0] - 1)
    early_kernel(
        inputs.at[pl.ds(0, 1)], others[0], inputs.at[rest], *others[1:], mixing, *plain,
        inputs_out.at[pl.ds(0, 1)], others_out[0], inputs_out.at[rest], *others_out[1:], semaphores,
    )


def relay_kernel(made_ref, passed_ref, out_ref):
    @pl.when(lax.axis_index("section") == 0)
    def _():
        out_ref[...] = made_ref[...]

    @pl.when(lax.axis_index("section") != 0)
    def _():
        out_ref[...] = passed_ref[...]


def relay_call(made, passed):
    return pl.pallas_call(
        relay_kernel,
        out_shape=jax.ShapeDtypeStruct(made.shape, made.dtype),
        in_specs=[VMEM, VMEM],
        out_specs=VMEM,
        compiler_params=pltpu.CompilerParams(vmem_limit_bytes=SCOPED_BYTES),
        name="relay",
    )(made, passed)


def firsts_kernel(inputs_ref, wv_ref, _token, *out_refs):
    @pl.when(lax.axis_index("section") == 0)
    def _():
        for micro, out_ref in enumerate(out_refs):
            out_ref[...] = first_values(inputs_ref[micro + 1], wv_ref[...])


def firsts_call(inputs, w_value, token):
    micro_count, row_count, _ = inputs.shape
    return pl.pallas_call(
        firsts_kernel,
        out_shape=[jax.ShapeDtypeStruct((row_count, w_value.shape[1]), jnp.bfloat16)]
        * (micro_count - 1),
        in_specs=[VMEM, VMEM, ANY],
        out_specs=[VMEM] * (micro_count - 1),
        compiler_params=pltpu.CompilerParams(vmem_limit_bytes=SCOPED_BYTES),
        name="firsts",
    )(inputs, w_value, token)


def layer_kernel(step, chunk, rows, layout, *refs):
    it = iter(refs)
    take = lambda count: [next(it) for _ in range(count)]
    micro_count, final, owners = layout
    inputs_ref, received_ref, mix_ref, _ = take(4)
    weights = take(4)
    first_refs = take(len(owners))
    earlier_refs = take(2 * chunk)
    home_refs = take(CHUNKS * (micro_count - 1)) if final and chunk == 0 else []
    take(1)
    if final:
        output_ref = take(1)[0]
    else:
        sent_ref = take(1)[0]
    take(1)
    if chunk + 1 < CHUNKS:
        keys_ref, used_ref = take(2)
    if final:
        rows_ref, semaphore = take(2)
    section = lax.axis_index("section")
    micro = step - section
    width = inputs_ref.shape[-1]
    active = jnp.logical_and(micro >= 0, micro < micro_count)
    span = slice(chunk * rows, (chunk + 1) * rows)

    @pl.when(active)
    def _():
        is_first = section == 0
        fresh = inputs_ref[min(step, micro_count - 1), span, :]
        hidden = jnp.where(is_first, fresh, received_ref[...])
        first = jnp.zeros((rows, weights[2].shape[1]), jnp.bfloat16)
        for index, (ref, sections) in enumerate(zip(first_refs, owners)):
            if index == 0:
                first = ref[span, :]
                continue
            mine = functools.reduce(jnp.logical_or, [section == s for s in sections])
            first = jnp.where(mine, ref[span, :], first)
        earlier = [ref[...] for ref in earlier_refs] or None
        hidden, keys, used = layer_chunk(
            hidden, first, is_first, mix_ref[0:1, 0:1], weights, earlier
        )
        if final:
            rows_ref[...] = hidden
            copy = pltpu.make_async_copy(
                rows_ref, output_ref.at[pl.ds(chunk * rows, rows)], semaphore
            )
            copy.start()
            copy.wait()
        else:
            sent_ref[...] = hidden
        if chunk + 1 < CHUNKS:
            keys_ref[...] = jnp.concatenate(keys, 1)
            used_ref[...] = used

    if final and chunk == 0:
        for home in range(micro_count - 1):

            @pl.when(section == home)
            def _():
                for part in range(CHUNKS):
                    move = pltpu.make_async_copy(
                        home_refs[CHUNKS * home + part],
                        output_ref.at[pl.ds(part * rows, rows)],
                        semaphore,
                    )
                    move.start()
                    move.wait()


def layer_call(step, chunk, rows, layout, operands, weights, firsts, earlier=(), extra=()):
    micro_count, final, owners = layout
    inputs, received = operands[:2]
    width, value_width = weights[0].shape
    kept = (rows, value_width)
    in_specs = [VMEM, VMEM, VMEM, ANY, VMEM, VMEM, VMEM, VMEM]
    in_specs += [VMEM] * (len(firsts) + len(earlier)) + [ANY] * len(extra)
    if final:
        out_shape = [jax.ShapeDtypeStruct((CHUNKS * rows, width), jnp.bfloat16)]
        out_specs = [ANY]
    else:
        out_shape = [jax.ShapeDtypeStruct((rows, width), jnp.bfloat16)]
        out_specs = [VMEM]
    out_shape.append(jax.ShapeDtypeStruct((8, 128), jnp.float32))
    out_specs.append(ANY)
    if chunk + 1 < CHUNKS:
        out_shape += [jax.ShapeDtypeStruct(kept, jnp.bfloat16)] * 2
        out_specs += [VMEM] * 2
    scratch = []
    if final:
        scratch += [pltpu.VMEM((rows, width), jnp.bfloat16), pltpu.SemaphoreType.DMA]
    aliases = {len(in_specs) - 1: 0} if final and chunk else {}
    return pl.pallas_call(
        functools.partial(layer_kernel, step, chunk, rows, layout),
        out_shape=out_shape,
        in_specs=in_specs,
        out_specs=out_specs,
        scratch_shapes=scratch,
        input_output_aliases=aliases,
        compiler_params=pltpu.CompilerParams(
            vmem_limit_bytes=SCOPED_BYTES
        ),
        cost_estimate=pl.CostEstimate(
            flops=8 * rows * width * value_width, bytes_accessed=0, transcendentals=0
        ),
        name="layer",
    )(*operands, *weights, *firsts, *earlier, *extra)


CHAIN = (0, 3, 2, 1, 5, 4, 7, 6)
LEAD = 2


def body(inputs, w_query, w_key, w_value, w_out, mixing):
    section_count = lax.axis_size("section")
    micro_count, row_count, width = inputs.shape
    last_section = section_count - 1
    last_step = micro_count + section_count - 2
    rows = row_count // CHUNKS
    last_hop = micro_count + section_count - 3
    first, mix, token, fresh, inputs, wv, wq, wk, wo = early_call(
        inputs, w_value[0], w_query[0], w_key[0], w_out[0], mixing, rows
    )
    received = [fresh] * CHUNKS
    made = [first]
    weights = (wq, wk, wv, wo)
    hops = []
    homes = []

    def hop(index):
        pairs = [
            (CHAIN[p], CHAIN[p + 1])
            for p in range(section_count - 1)
            if 0 <= index - p < micro_count
        ]
        if index == 0:
            given = made[0]
        elif index < micro_count:
            given = relay_call(made[index], hops[-1])
        else:
            given = hops[-1]
        hops.append(lax.ppermute(given, "section", pairs))
        return given

    hop(0)
    for step in range(last_step + 1):
        arrived = []
        kept = ()
        needed = {}
        for s in range(1, section_count):
            if 0 <= step - s < micro_count:
                needed.setdefault(step - s + CHAIN.index(s) - 1, []).append(s)
        owners = tuple(tuple(group) for group in needed.values())
        firsts = tuple(hops[index] for index in needed)
        passed = token
        if step >= 1 and step + LEAD <= last_hop:
            passed = hop(step + LEAD)
        for chunk in range(CHUNKS):
            final = step == last_step
            extra = (passed,) if chunk == 0 else (token,)
            if final:
                extra = tuple(homes) + (passed,) if chunk == 0 else (output,)
            results = layer_call(
                step, chunk, rows, (micro_count, final, owners),
                (inputs, received[chunk], mix, token), weights, firsts, kept, extra,
            )
            sent, token = results[:2]
            results = results[2:]
            if chunk + 1 < CHUNKS:
                kept += tuple(results[:2])
                results = results[2:]
            if final:
                output = sent
                continue
            pairs = [(s, s + 1) for s in range(last_section) if 0 <= step - s < micro_count]
            done = step - last_section
            if 0 <= done < last_section:
                pairs.append((last_section, done))
            arrived.append(lax.ppermute(sent, "section", pairs))
        if step == 0:
            made += firsts_call(inputs, wv, token)
            for index in range(1, LEAD + 1):
                hop(index)
        received = arrived
        if last_section <= step < last_step:
            homes += received
    return output[None]


def solution(mesh):
    in_specs = (
        P("dp", None, None),
        P("section", None, None),
        P("section", None, None),
        P("section", None, None),
        P("section", None, None),
        P("section"),
    )
    out_specs = P(("dp", "section"), None, None)
    return jax.shard_map(body, mesh=mesh, in_specs=in_specs, out_specs=out_specs, check_vma=False)
```

```python
import functools

import jax
import jax.numpy as jnp
from jax import lax
from jax.experimental import pallas as pl
from jax.experimental.pallas import tpu as pltpu
from jax.sharding import PartitionSpec as P

HEADS = 6
CHUNKS = 2
SHIFT = 2

epsilon = 1e-06
score_scale = 0.12


VMEM = pl.BlockSpec(memory_space=pltpu.VMEM)
ANY = pl.BlockSpec(memory_space=pl.ANY)
HBM = pl.BlockSpec(memory_space=pltpu.HBM)
SCOPED_BYTES = 8 * 1024 * 1024


def norm_rows(tensor):
    return tensor * lax.rsqrt(jnp.mean(tensor * tensor, axis=-1, keepdims=True) + epsilon)


def heads_of(tensor):
    head_dim = tensor.shape[-1] // HEADS
    return [tensor[:, head * head_dim : (head + 1) * head_dim] for head in range(HEADS)]


def dot(left, right):
    return jnp.dot(left, right, preferred_element_type=jnp.float32)


def layer_chunk(hidden, first, is_first, mix, weights, earlier):
    rows = hidden.shape[0]
    wq_ref, wk_ref, wv_ref, wo_ref = weights
    hidden_wide = hidden.astype(jnp.float32)
    normed = norm_rows(hidden_wide).astype(jnp.bfloat16)
    queries = dot(normed, wq_ref[...])
    key_rows = dot(normed, wk_ref[...])
    values = dot(normed, wv_ref[...])
    queries = [norm_rows(head).astype(jnp.bfloat16) for head in heads_of(queries)]
    keys = [norm_rows(head).astype(jnp.bfloat16) for head in heads_of(key_rows)]
    own = values.astype(jnp.bfloat16)
    blended = (mix * values + (1.0 - mix) * first.astype(jnp.float32)).astype(jnp.bfloat16)
    used = jnp.where(is_first, own, blended)
    all_keys, all_used = keys, heads_of(used)
    if earlier is not None:
        all_keys = [jnp.concatenate(pair, 0) for pair in zip(heads_of(earlier[0]), keys)]
        all_used = [jnp.concatenate(pair, 0) for pair in zip(heads_of(earlier[1]), all_used)]
    scores = [
        lax.dot_general(query, key, (((1,), (1,)), ((), ())), preferred_element_type=jnp.float32)
        for query, key in zip(queries, all_keys)
    ]
    count = all_keys[0].shape[0]
    row_ids = lax.broadcasted_iota(jnp.int32, (rows, count), 0) + (count - rows)
    causal = row_ids >= lax.broadcasted_iota(jnp.int32, (rows, count), 1)
    masses = [jnp.where(causal, jnp.exp(score * score_scale), 0.0) for score in scores]
    totals = [jnp.sum(mass, axis=-1, keepdims=True) for mass in masses]
    shares = [(mass / total).astype(jnp.bfloat16) for mass, total in zip(masses, totals)]
    attended = [dot(share, value).astype(jnp.bfloat16) for share, value in zip(shares, all_used)]
    projected = dot(jnp.concatenate(attended, 1), wo_ref[...])
    return (hidden_wide + projected).astype(jnp.bfloat16), keys, used


def first_values(rows, wv):
    return dot(norm_rows(rows.astype(jnp.float32)).astype(jnp.bfloat16), wv).astype(jnp.bfloat16)


def early_kernel(*refs):
    sources, mixing_ref = refs[:5], refs[5]
    mix_ref, _token, _received = refs[6:9]
    targets, semaphores = refs[9:14], refs[14]
    copies = [
        pltpu.make_async_copy(source, target, semaphores.at[index])
        for index, (source, target) in enumerate(zip(sources, targets))
    ]
    for copy in copies:
        copy.start()
    mix_ref[...] = jnp.full(mix_ref.shape, mixing_ref[0])
    for copy in copies:
        copy.wait()


def early_call(loaded, mixing, rows):
    width = loaded[0].shape[-1]
    return pl.pallas_call(
        early_kernel,
        out_shape=[
            pltpu.VMEM((8, 128), jnp.float32),
            jax.ShapeDtypeStruct((8, 128), jnp.float32),
            pltpu.VMEM((rows, width), jnp.bfloat16),
        ]
        + [pltpu.VMEM(w.shape, w.dtype) for w in loaded],
        in_specs=[HBM] * 5 + [pl.BlockSpec(memory_space=pltpu.SMEM)],
        out_specs=[VMEM, ANY, VMEM] + [VMEM] * 5,
        scratch_shapes=[pltpu.SemaphoreType.DMA((5,))],
        compiler_params=pltpu.CompilerParams(vmem_limit_bytes=50 * 1024 * 1024),
        name="early",
    )(*loaded, mixing)


def relay_kernel(made_ref, passed_ref, out_ref):
    @pl.when(lax.axis_index("section") == 0)
    def _():
        out_ref[...] = made_ref[...]

    @pl.when(lax.axis_index("section") != 0)
    def _():
        out_ref[...] = passed_ref[...]


def relay_call(made, passed):
    return pl.pallas_call(
        relay_kernel,
        out_shape=jax.ShapeDtypeStruct(made.shape, made.dtype),
        in_specs=[VMEM, VMEM],
        out_specs=VMEM,
        compiler_params=pltpu.CompilerParams(vmem_limit_bytes=SCOPED_BYTES),
        name="relay",
    )(made, passed)


def firsts_kernel(inputs_ref, wv_ref, _token, *out_refs):
    @pl.when(lax.axis_index("section") == 0)
    def _():
        for micro, out_ref in enumerate(out_refs):
            out_ref[...] = first_values(inputs_ref[micro], wv_ref[...])


def firsts_call(inputs, w_value, token):
    micro_count, row_count, _ = inputs.shape
    return pl.pallas_call(
        firsts_kernel,
        out_shape=[jax.ShapeDtypeStruct((row_count, w_value.shape[1]), jnp.bfloat16)]
        * micro_count,
        in_specs=[VMEM, VMEM, ANY],
        out_specs=[VMEM] * micro_count,
        compiler_params=pltpu.CompilerParams(vmem_limit_bytes=SCOPED_BYTES),
        name="firsts",
    )(inputs, w_value, token)


def layer_kernel(step, chunk, rows, layout, *refs):
    it = iter(refs)
    take = lambda count: [next(it) for _ in range(count)]
    micro_count, final, owners = layout
    inputs_ref, received_ref, mix_ref, _ = take(4)
    weights = take(4)
    first_refs = take(len(owners))
    earlier_refs = take(2 * chunk)
    home_refs = take(CHUNKS * (micro_count - 1)) if final and chunk == 0 else []
    take(1)
    if final:
        output_ref = take(1)[0]
    else:
        sent_ref = take(1)[0]
    take(1)
    if chunk + 1 < CHUNKS:
        keys_ref, used_ref = take(2)
    if final:
        rows_ref, semaphore = take(2)
    section = lax.axis_index("section")
    micro = step - SHIFT * section
    width = inputs_ref.shape[-1]
    active = jnp.logical_and(micro >= 0, micro < micro_count)
    span = slice(chunk * rows, (chunk + 1) * rows)

    @pl.when(active)
    def _():
        is_first = section == 0
        fresh = inputs_ref[min(step, micro_count - 1), span, :]
        hidden = jnp.where(is_first, fresh, received_ref[:, :width])
        if received_ref.shape[1] > width:
            first = received_ref[:, width:]
        else:
            first = jnp.zeros((rows, weights[2].shape[1]), jnp.bfloat16)
        for index, (ref, sections) in enumerate(zip(first_refs, owners)):
            if index == 0:
                first = ref[span, :]
                continue
            mine = functools.reduce(jnp.logical_or, [section == s for s in sections])
            first = jnp.where(mine, ref[span, :], first)
        earlier = [ref[...] for ref in earlier_refs] or None
        hidden, keys, used = layer_chunk(
            hidden, first, is_first, mix_ref[0:1, 0:1], weights, earlier
        )
        if final:
            rows_ref[...] = hidden
            copy = pltpu.make_async_copy(
                rows_ref, output_ref.at[pl.ds(chunk * rows, rows)], semaphore
            )
            copy.start()
            copy.wait()
        else:
            sent_ref[:, :width] = hidden
            if sent_ref.shape[1] > width:
                sent_ref[:, width:] = used
        if chunk + 1 < CHUNKS:
            keys_ref[...] = jnp.concatenate(keys, 1)
            used_ref[...] = used

    if final and chunk == 0:
        for home in range(micro_count - 1):

            @pl.when(section == home)
            def _():
                for part in range(CHUNKS):
                    move = pltpu.make_async_copy(
                        home_refs[CHUNKS * home + part],
                        output_ref.at[pl.ds(part * rows, rows)],
                        semaphore,
                    )
                    move.start()
                    move.wait()


def layer_call(step, chunk, rows, layout, operands, weights, firsts, earlier=(), extra=()):
    micro_count, final, owners = layout
    inputs, received = operands[:2]
    width, value_width = weights[0].shape
    kept = (rows, value_width)
    in_specs = [VMEM, VMEM, VMEM, ANY, VMEM, VMEM, VMEM, VMEM]
    in_specs += [VMEM] * (len(firsts) + len(earlier)) + [ANY] * len(extra)
    if final:
        out_shape = [jax.ShapeDtypeStruct((CHUNKS * rows, width), jnp.bfloat16)]
        out_specs = [ANY]
    else:
        wide = value_width if step < SHIFT else 0
        out_shape = [jax.ShapeDtypeStruct((rows, width + wide), jnp.bfloat16)]
        out_specs = [VMEM]
    out_shape.append(jax.ShapeDtypeStruct((8, 128), jnp.float32))
    out_specs.append(ANY)
    if chunk + 1 < CHUNKS:
        out_shape += [jax.ShapeDtypeStruct(kept, jnp.bfloat16)] * 2
        out_specs += [VMEM] * 2
    scratch = []
    if final:
        scratch += [pltpu.VMEM((rows, width), jnp.bfloat16), pltpu.SemaphoreType.DMA]
    aliases = {len(in_specs) - 1: 0} if final and chunk else {}
    return pl.pallas_call(
        functools.partial(layer_kernel, step, chunk, rows, layout),
        out_shape=out_shape,
        in_specs=in_specs,
        out_specs=out_specs,
        scratch_shapes=scratch,
        input_output_aliases=aliases,
        compiler_params=pltpu.CompilerParams(
            vmem_limit_bytes=SCOPED_BYTES
        ),
        cost_estimate=pl.CostEstimate(
            flops=8 * rows * width * value_width, bytes_accessed=0, transcendentals=0
        ),
        name="layer",
    )(*operands, *weights, *firsts, *earlier, *extra)


CHAIN = (0, 3, 2, 1, 5, 4, 7, 6)


def body(inputs, w_query, w_key, w_value, w_out, mixing):
    section_count = lax.axis_size("section")
    micro_count, row_count, width = inputs.shape
    last_section = section_count - 1
    last_step = micro_count - 1 + SHIFT * last_section
    rows = row_count // CHUNKS
    last_hop = micro_count + section_count - 3
    loaded = (inputs, w_query[0], w_key[0], w_value[0], w_out[0])
    mix, token, unset, inputs, wq, wk, wv, wo = early_call(loaded, mixing, rows)
    weights = (wq, wk, wv, wo)
    pending = [[unset] * CHUNKS] * SHIFT
    made = []
    hops = []
    homes = []

    def hop():
        index = len(hops)
        if index == 0:
            given = made[0]
        elif index < micro_count:
            given = relay_call(made[index], hops[-1])
        else:
            given = hops[-1]
        hops.append(lax.ppermute(given, "section", list(zip(CHAIN[:-1], CHAIN[1:]))))
        return given

    for step in range(last_step + 1):
        final = step == last_step
        arrived = []
        kept = ()
        needed = {}
        for s in range(1, section_count):
            if 0 <= step - SHIFT * s < micro_count and step >= 2 * SHIFT:
                needed.setdefault(step - SHIFT * s + CHAIN.index(s) - 1, []).append(s)
        owners = tuple(tuple(group) for group in needed.values())
        firsts = tuple(hops[index] for index in needed)
        passed = hop() if 1 <= step and len(hops) <= last_hop else token
        received = pending.pop(0)
        for chunk in range(CHUNKS):
            if step == 1 and chunk == 1:
                passed = hop()
            extra = (passed,)
            if final:
                extra = tuple(homes) + (passed,) if chunk == 0 else (output,)
            results = layer_call(
                step, chunk, rows, (micro_count, final, owners),
                (inputs, received[chunk], mix, token), weights, firsts, kept, extra,
            )
            sent, token = results[:2]
            if chunk + 1 < CHUNKS:
                kept += tuple(results[2:4])
            if final:
                output = sent
                continue
            done = step - SHIFT * last_section
            if done < 0:
                pairs = [(s, s + 1) for s in range(last_section)]
            else:
                pairs = [
                    (s, s + 1) for s in range(last_section) if 0 <= step - SHIFT * s < micro_count
                ]
                pairs.append((last_section, done))
            arrived.append(lax.ppermute(sent, "section", pairs))
        if step == 0:
            made = firsts_call(inputs, wv, token)
            hop()
        pending.append(arrived)
        if SHIFT * last_section <= step < last_step:
            homes += arrived
    return output[None]


def solution(mesh):
    in_specs = (
        P("dp", None, None),
        P("section", None, None),
        P("section", None, None),
        P("section", None, None),
        P("section", None, None),
        P("section"),
    )
    out_specs = P(("dp", "section"), None, None)
    return jax.shard_map(body, mesh=mesh, in_specs=in_specs, out_specs=out_specs, check_vma=False)
```
